32 devices in a mesh: cells: 8 (over z, y), coef: 4 (over x, core).
Axes of the slice: x: 2, y: 2, z: 4, core: 2. Of those that a mesh axis runs over, the one named last changes fastest.
Arguments:
- multipole: bfloat16 [128, 1024], P('coef', 'cells'), may hold values from -6 to 6
- parent_local: bfloat16 [128, 128], P('coef', 'cells'), may hold values from -6 to 6
- m2l_ops: bfloat16 [189, 128, 128], P(None, 'coef'), may hold values from -0.0390625 to 0.0390625
- l2l_ops: bfloat16 [8, 128, 128], P(None, 'coef'), may hold values from -0.5 to 0.5
- target_cell: int32 [189, 1024], P(None, 'cells'), may hold values from -1 to 1023, as said below
- particle_leaf: int32 [16384], P('cells'), may hold values from 0 to 1023, as said below
- particle_basis: bfloat16 [128, 16384], P('coef', 'cells'), may hold values from -0.5 to 0.5
Outputs:
- leaf_local: float32 [128, 1024], P('coef', 'cells')
- potential: float32 [16384], P('cells')
The draws below stay inside these ranges and needn't reach their ends.
Inputs may be any that keep to these rules, and one draw needn't show every extreme that they name: `target_cell`: -1 marks an empty slot. Otherwise the target of source cell c lies on the device of c (cells are owned in blocks of 128: device c // 128) or on a device at most 2 indices away; from one device's source cells at most 256 pairs target the cells of any one other device, and some pair of devices has exactly 256. `particle_leaf`: the particles at positions d * 2048 to (d + 1) * 2048 - 1 lie in cells d * 128 to (d + 1) * 128 - 1.
All inputs are finite; a program needn't handle non-finite values.
Results may differ from the reference program's by a relative error of at most 0.0003.
Values may be sent and summed in bfloat16 or wider, within the bound.
No kernel may reach another device: no remote copies, remote signals or barrier semaphores. Data moves between devices by JAX's collectives and lax.ppermute only.
A program may use at most 64 MiB of HBM per device.

```python
import jax
import jax.numpy as jnp
import numpy as np
from jax import lax

K = 128
NOFF = 189
CD = 128
PD = 2048
CAP = 256
REACH = 2
OWNERS = 8
CELLS = 1024
PCELLS = 128
PARTICLES = 16384


def draw_target_cell(key, part):
    moves = jnp.asarray(np.concatenate([np.arange(-REACH, 0), np.arange(1, REACH + 1)]), jnp.int32)
    groups = 2 * REACH
    pairs = NOFF * CD

    def one_device(device):
        device_key = jax.random.fold_in(jax.random.fold_in(key, 11), device)
        keys = jax.random.split(device_key, 5)
        counts = jax.random.randint(keys[0], (groups,), CAP // 4, CAP + 1)
        forced = jax.random.randint(keys[1], (), 0, groups)
        counts = jnp.where(jnp.arange(groups) == forced, CAP, counts)
        dests = device + moves
        inside = (dests >= 0) & (dests < OWNERS)
        counts = jnp.where(inside, counts, 0).astype(jnp.int32)
        ends = jnp.cumsum(counts).astype(jnp.int32)
        order = jax.random.permutation(keys[2], pairs)
        place = jnp.zeros((pairs,), jnp.int32).at[order].set(jnp.arange(pairs, dtype=jnp.int32))
        group = jnp.searchsorted(ends, place, side='right').astype(jnp.int32)
        remote = group < groups
        target_dev = device + moves[jnp.minimum(group, groups - 1)]
        cell = jax.random.randint(keys[3], (pairs,), 0, CD)
        empty = jax.random.randint(keys[4], (pairs,), 0, 8) == 0
        local_target = jnp.where(empty, -1, device * CD + cell)
        result = jnp.where(remote, target_dev * CD + cell, local_target)
        return result.astype(jnp.int32).reshape(NOFF, CD)
    table = lax.map(one_device, jnp.arange(OWNERS, dtype=jnp.int32))
    return jnp.transpose(table, (1, 0, 2)).reshape(NOFF, OWNERS * CD)


def draw_particle_leaf(key, part):
    leaf_key = jax.random.fold_in(key, 23)
    owner = jnp.arange(PD * OWNERS, dtype=jnp.int32) // PD
    cell = jax.random.randint(leaf_key, (PD * OWNERS,), 0, CD)
    return (owner * CD + cell).astype(jnp.int32)


def block_scale(own_key, extent, pieces, smallest, largest):
    gain = 1.0
    for dim, parts in pieces:
        steps = jax.random.uniform(jax.random.fold_in(jax.random.fold_in(own_key, 6), dim), (parts,), jnp.float32, smallest / len(pieces), largest / len(pieces))
        gain = gain * jnp.repeat(jnp.exp(steps), extent[dim] // parts).reshape((-1,) + (1,) * (len(extent) - 1 - dim))
    return gain


def normal_values(stream_key, dims, scale, bound, shards=(), kind=jnp.bfloat16):
    loudness = block_scale(stream_key, dims, shards, -0.22, 0.18) if shards else 1.0
    values = jax.random.normal(stream_key, dims, jnp.float32) * scale * loudness
    return jnp.minimum(jnp.maximum(values, -bound), bound).astype(kind)


def setup_inputs(seed: int = 0) -> dict:
    key_list = jax.random.split(jax.random.key(seed), 8)
    multipole = normal_values(key_list[0], (K, CELLS), 1.0, 6.0, ((0, 4), (1, 8)))
    parent_local = normal_values(key_list[1], (K, PCELLS), 1.0, 6.0, ((0, 4), (1, 8)))
    m2l_ops = normal_values(key_list[2], (NOFF, K, K), (K * NOFF) ** -0.5, 0.0390625, ((1, 4),))
    l2l_ops = normal_values(key_list[3], (8, K, K), K ** -0.5, 0.5, ((1, 4),))
    target_cell = draw_target_cell(jax.random.fold_in(key_list[7], 71), 0)
    particle_leaf = draw_particle_leaf(jax.random.fold_in(key_list[7], 71), 0)
    particle_basis = normal_values(key_list[6], (K, PARTICLES), K ** -0.5, 0.5, ((0, 4), (1, 8)))
    return dict(multipole=multipole, parent_local=parent_local, m2l_ops=m2l_ops, l2l_ops=l2l_ops, target_cell=target_cell, particle_leaf=particle_leaf, particle_basis=particle_basis)


def reference(multipole, parent_local, m2l_ops, l2l_ops, target_cell, particle_leaf, particle_basis):
    width = multipole.shape[0]
    cell_count = multipole.shape[1]
    poles_wide = multipole.astype(jnp.float32)
    parents_wide = parent_local.astype(jnp.float32)

    def offset_step(total, inputs):
        operator, targets = inputs
        term = jnp.dot(operator.astype(jnp.float32), poles_wide, preferred_element_type=jnp.float32)
        index = jnp.where(targets >= 0, targets, cell_count).astype(jnp.int32)
        return total.at[:, index].add(term, mode="drop"), None

    start = jnp.zeros((width, cell_count), jnp.float32)
    m2l_sum, _ = lax.scan(offset_step, start, (m2l_ops, target_cell))
    children = [jnp.dot(l2l_ops[octant].astype(jnp.float32), parents_wide, preferred_element_type=jnp.float32) for octant in range(8)]
    shifted = jnp.stack(children, axis=2).reshape(width, cell_count)
    leaf_local = m2l_sum + shifted
    columns = leaf_local[:, particle_leaf]
    potential = jnp.sum(columns * particle_basis.astype(jnp.float32), axis=0)
    return leaf_local, potential
```

```python
import functools

import jax
import jax.numpy as jnp
from jax import lax
from jax.experimental import pallas as pl
from jax.experimental.pallas import tpu as pltpu
from jax.sharding import PartitionSpec as P

REACH = 2
BLOCKS = 2 * REACH + 1
GROUP = 8


def far_kernel(ops_ref, full_ref, tgt_ref, l2l_ref, *refs, share, cells, parents, noff):
    outs = refs[:BLOCKS]
    poles_t, hot, rhs, acc = refs[BLOCKS:]
    f32, bf16 = jnp.float32, jnp.bfloat16
    lanes = 4 * share
    poles_t[...] = full_ref[:, :cells].astype(f32).T.astype(bf16)
    acc[...] = jnp.zeros_like(acc)
    rows = lax.broadcasted_iota(jnp.int32, (cells, cells), 0).astype(f32).astype(bf16)
    lane = lax.broadcasted_iota(jnp.int32, (cells, lanes), 1)
    is_high = (lane % (2 * share)) < share
    is_even = lane < 2 * share
    one = jnp.ones((cells, cells), bf16)
    zero = jnp.zeros((cells, cells), bf16)

    def chunk(first, count):
        wide = tgt_ref[pl.ds(first, count), :]
        for b in range(BLOCKS):
            local = jnp.clip(wide - b * cells, -1, cells).astype(f32)
            for j in range(count):
                row = jnp.broadcast_to(local[j : j + 1, :], (cells, cells)).astype(bf16)
                hot[b * cells : (b + 1) * cells, j * cells : (j + 1) * cells] = jnp.where(
                    row == rows, one, zero
                )
        for j in range(0, count, 2):
            pair = min(2, count - j)
            parts = []
            for i in range(2):
                op = ops_ref[first + j + min(i, pair - 1)]
                parts += [op, op]
            weights = jnp.concatenate(parts, axis=0)
            term = lax.dot_general(
                poles_t[...], weights, (((1,), (1,)), ((), ())), preferred_element_type=f32
            )
            high = term.astype(bf16).astype(f32)
            both = jnp.where(is_high, high, term - high)
            rhs[j * cells : (j + 1) * cells, :] = jnp.where(is_even, both, 0.0).astype(bf16)
            if pair == 2:
                rhs[(j + 1) * cells : (j + 2) * cells, :] = jnp.where(is_even, 0.0, both).astype(bf16)
        width = count * cells
        acc[...] += jnp.dot(hot[:, :width], rhs[:width, :], preferred_element_type=f32)

    whole = noff // GROUP

    def step(i, carry):
        chunk(pl.multiple_of(i * GROUP, GROUP), GROUP)
        return carry

    lax.fori_loop(0, whole, step, 0)
    if noff % GROUP:
        chunk(whole * GROUP, noff % GROUP)

    parent = full_ref[:, cells:]
    width = parent.shape[1]
    src = lax.broadcasted_iota(jnp.int32, (width, cells), 0)
    dst = lax.broadcasted_iota(jnp.int32, (width, cells), 1)
    children = cells // parents
    spread = jnp.where(dst // children == src, 1.0, 0.0).astype(bf16)
    rep = jnp.dot(parent, spread, preferred_element_type=f32)
    octant = lax.broadcasted_iota(jnp.int32, rep.shape, 1) % children
    shifted = jnp.zeros((share, cells), f32)
    for o in range(children):
        chosen = jnp.where(octant == o, rep, 0.0).astype(bf16)
        shifted = shifted + jnp.dot(l2l_ref[o], chosen, preferred_element_type=f32)

    for b in range(BLOCKS):
        t = acc[b * cells : (b + 1) * cells, :].T
        t = (t[:share] + t[share : 2 * share]) + (t[2 * share : 3 * share] + t[3 * share :])
        outs[b][...] = t + shifted if b == REACH else t


def near_kernel(*refs, share, cells):
    pieces = refs[:BLOCKS]
    leaf_ref, basis_ref, out_ref, pot_ref = refs[BLOCKS:]
    f32, bf16 = jnp.float32, jnp.bfloat16
    leaf = pieces[0][...]
    for piece in pieces[1:]:
        leaf = leaf + piece[...]
    out_ref[...] = leaf
    high = leaf.astype(bf16)
    low = (leaf - high.astype(f32)).astype(bf16)
    both = jnp.concatenate([high, low], axis=0)
    count = leaf_ref.shape[1]
    rows = lax.broadcasted_iota(jnp.int32, (cells, count), 0)
    hot = jnp.where(rows == leaf_ref[...], 1.0, 0.0).astype(bf16)
    columns = jnp.dot(both, hot, preferred_element_type=f32)
    columns = columns[:share] + columns[share:]
    pot_ref[...] = jnp.sum(columns * basis_ref[...].astype(f32), axis=0, keepdims=True)


def passed_along(value, axis, steps):
    count = lax.axis_size(axis)
    first, last = (max(0, -steps), min(count, count - steps))
    return lax.ppermute(value, axis, [(source, source + steps) for source in range(first, last)])


def on_device(
    multipole, parent_local, m2l_ops, l2l_ops, target_cell, particle_leaf, particle_basis
):
    my_index = lax.axis_index("cells")
    cells = multipole.shape[1]
    parents = parent_local.shape[1]
    noff, share, width = m2l_ops.shape
    pad = -parents % 128
    joined = jnp.concatenate(
        [multipole, parent_local, jnp.zeros((multipole.shape[0], pad), multipole.dtype)], axis=1
    )
    full = lax.all_gather(joined, "coef", axis=0, tiled=True)
    span = BLOCKS * cells
    lowest = (my_index - REACH) * cells
    wide = jnp.where(target_cell >= 0, target_cell - lowest, span)
    vmem = pl.BlockSpec(memory_space=pltpu.VMEM)
    blocks = pl.pallas_call(
        functools.partial(far_kernel, share=share, cells=cells, parents=parents, noff=noff),
        out_shape=[jax.ShapeDtypeStruct((share, cells), jnp.float32)] * BLOCKS,
        in_specs=[vmem] * 4,
        out_specs=[vmem] * BLOCKS,
        scratch_shapes=[
            pltpu.VMEM((cells, width), jnp.bfloat16),
            pltpu.VMEM((span, GROUP * cells), jnp.bfloat16),
            pltpu.VMEM((GROUP * cells, 4 * share), jnp.bfloat16),
            pltpu.VMEM((span, 4 * share), jnp.float32),
        ],
        name="far",
    )(m2l_ops, full, wide, l2l_ops)
    pieces = [blocks[REACH]]
    for length in range(1, REACH + 1):
        for direction in (1, -1):
            distance = length * direction
            pieces.append(passed_along(blocks[REACH + distance], "cells", distance))
    index = (particle_leaf - my_index * cells).reshape(1, -1)
    count = index.shape[1]
    leaf_local, partial = pl.pallas_call(
        functools.partial(near_kernel, share=share, cells=cells),
        out_shape=[
            jax.ShapeDtypeStruct((share, cells), jnp.float32),
            jax.ShapeDtypeStruct((1, count), jnp.float32),
        ],
        in_specs=[vmem] * (BLOCKS + 2),
        out_specs=[vmem] * 2,
        name="near",
    )(*pieces, index, particle_basis)
    potential = lax.psum(partial.reshape(-1), "coef")
    return (leaf_local, potential)


def solution(mesh):
    return jax.shard_map(
        on_device,
        mesh=mesh,
        in_specs=(
            P("coef", "cells"),
            P("coef", "cells"),
            P(None, "coef", None),
            P(None, "coef", None),
            P(None, "cells"),
            P("cells"),
            P("coef", "cells"),
        ),
        out_specs=(P("coef", "cells"), P("cells")),
        check_vma=False,
    )
```

```python
import functools

import jax
import jax.numpy as jnp
from jax import lax
from jax.experimental import pallas as pl
from jax.experimental.pallas import tpu as pltpu
from jax.sharding import PartitionSpec as P

REACH = 2
BLOCKS = 2 * REACH + 1
GROUP = 8


def swap_steps(index):
    steps = []
    for length in range(1, REACH + 1):
        side = (index // length) % 2
        steps += [length * (1 - 2 * side), length * (2 * side - 1)]
    return steps


def far_kernel(*refs, share, cells, parents, noff, coefs):
    f32, bf16 = jnp.float32, jnp.bfloat16
    shards = refs[:coefs]
    ops_ref, tgt_ref, l2l_ref = refs[coefs : coefs + 3]
    outs = refs[coefs + 3 : coefs + 3 + BLOCKS]
    poles, spread_parents, poles_t, hot, rhs, acc = refs[coefs + 3 + BLOCKS :]
    cell_index = lax.axis_index("cells")
    coef_index = lax.axis_index("coef")
    lowest = (cell_index - REACH) * cells
    lanes = 4 * share
    children = cells // parents
    src = lax.broadcasted_iota(jnp.int32, (parents, cells), 0)
    dst = lax.broadcasted_iota(jnp.int32, (parents, cells), 1)
    spread = jnp.where(dst // children == src, 1.0, 0.0).astype(bf16)
    for k in range(coefs):
        at = pl.multiple_of((coef_index ^ k) * share, share)
        shard = shards[k][...]
        poles[pl.ds(at, share), :] = shard[:share, :]
        spread_parents[pl.ds(at, share), :] = lax.dot_general(
            shard[share:, :], spread, (((0,), (0,)), ((), ())), preferred_element_type=f32
        )[:share]
    poles_t[...] = poles[...].astype(f32).T.astype(bf16)
    acc[...] = jnp.zeros_like(acc)
    rows = lax.broadcasted_iota(jnp.int32, (cells, cells), 0).astype(f32).astype(bf16)
    lane = lax.broadcasted_iota(jnp.int32, (cells, lanes), 1)
    is_high = (lane % (2 * share)) < share
    is_even = lane < 2 * share
    one = jnp.ones((cells, cells), bf16)
    zero = jnp.zeros((cells, cells), bf16)

    def chunk(first, count):
        target = tgt_ref[pl.ds(first, count), :]
        wide = jnp.where(target >= 0, target - lowest, -1)
        for b in range(BLOCKS):
            local = jnp.clip(wide - b * cells, -1, cells).astype(f32)
            for j in range(count):
                row = jnp.broadcast_to(local[j : j + 1, :], (cells, cells)).astype(bf16)
                hot[b * cells : (b + 1) * cells, j * cells : (j + 1) * cells] = jnp.where(
                    row == rows, one, zero
                )
        for j in range(0, count, 2):
            pair = min(2, count - j)
            parts = []
            for i in range(2):
                op = ops_ref[first + j + min(i, pair - 1)]
                parts += [op, op]
            weights = jnp.concatenate(parts, axis=0)
            term = lax.dot_general(
                poles_t[...], weights, (((1,), (1,)), ((), ())), preferred_element_type=f32
            )
            high = term.astype(bf16).astype(f32)
            both = jnp.where(is_high, high, term - high)
            rhs[j * cells : (j + 1) * cells, :] = jnp.where(is_even, both, 0.0).astype(bf16)
            if pair == 2:
                rhs[(j + 1) * cells : (j + 2) * cells, :] = jnp.where(is_even, 0.0, both).astype(bf16)
        width = count * cells
        acc[...] += jnp.dot(hot[:, :width], rhs[:width, :], preferred_element_type=f32)

    whole = noff // GROUP

    def step(i, carry):
        chunk(pl.multiple_of(i * GROUP, GROUP), GROUP)
        return carry

    lax.fori_loop(0, whole, step, 0)
    if noff % GROUP:
        chunk(whole * GROUP, noff % GROUP)

    rep = spread_parents[...]
    octant = lax.broadcasted_iota(jnp.int32, rep.shape, 1) % children
    shifted = jnp.zeros((share, cells), f32)
    for o in range(children):
        chosen = jnp.where(octant == o, rep, 0.0).astype(bf16)
        shifted = shifted + jnp.dot(l2l_ref[o], chosen, preferred_element_type=f32)

    steps = [0] + swap_steps(cell_index)
    for out, step in zip(outs, steps):
        at = pl.multiple_of((REACH + step) * cells, cells)
        t = acc[pl.ds(at, cells), :].T
        t = (t[:share] + t[share : 2 * share]) + (t[2 * share : 3 * share] + t[3 * share :])
        out[...] = t if out is not outs[0] else t + shifted


def near_kernel(*refs, share, cells):
    pieces = refs[:BLOCKS]
    leaf_ref, basis_ref, out_ref, pot_ref = refs[BLOCKS:]
    f32, bf16 = jnp.float32, jnp.bfloat16
    leaf = pieces[0][...]
    for piece in pieces[1:]:
        leaf = leaf + piece[...]
    out_ref[...] = leaf
    high = leaf.astype(bf16)
    low = (leaf - high.astype(f32)).astype(bf16)
    both = jnp.concatenate([high, low], axis=0)
    count = leaf_ref.shape[1]
    rows = lax.broadcasted_iota(jnp.int32, (cells, count), 0)
    hot = jnp.where(rows == leaf_ref[...], 1.0, 0.0).astype(bf16)
    columns = jnp.dot(both, hot, preferred_element_type=f32)
    columns = columns[:share] + columns[share:]
    pot_ref[...] = jnp.sum(columns * basis_ref[...].astype(f32), axis=0, keepdims=True)


def swapped(value, length, phase):
    count = lax.axis_size("cells")
    pairs = []
    for low in range(count - length):
        if (low // length) % 2 == phase:
            pairs += [(low, low + length), (low + length, low)]
    return lax.ppermute(value, "cells", pairs)


def from_all(value):
    count = lax.axis_size("coef")
    return [value] + [
        lax.ppermute(value, "coef", [(i, i ^ k) for i in range(count)]) for k in range(1, count)
    ]


def on_device(
    multipole, parent_local, m2l_ops, l2l_ops, target_cell, particle_leaf, particle_basis
):
    my_index = lax.axis_index("cells")
    cells = multipole.shape[1]
    parents = parent_local.shape[1]
    coefs = lax.axis_size("coef")
    noff, share, width = m2l_ops.shape
    flipped = jnp.pad(parent_local.T, ((0, 0), (0, cells - share)))
    shards = from_all(jnp.concatenate([multipole, flipped], axis=0))
    span = BLOCKS * cells
    vmem = pl.BlockSpec(memory_space=pltpu.VMEM)
    blocks = pl.pallas_call(
        functools.partial(
            far_kernel, share=share, cells=cells, parents=parents, noff=noff, coefs=coefs
        ),
        out_shape=[jax.ShapeDtypeStruct((share, cells), jnp.float32)] * BLOCKS,
        in_specs=[vmem] * (coefs + 3),
        out_specs=[vmem] * BLOCKS,
        scratch_shapes=[
            pltpu.VMEM((width, cells), jnp.bfloat16),
            pltpu.VMEM((width, cells), jnp.float32),
            pltpu.VMEM((cells, width), jnp.bfloat16),
            pltpu.VMEM((span, GROUP * cells), jnp.bfloat16),
            pltpu.VMEM((GROUP * cells, 4 * share), jnp.bfloat16),
            pltpu.VMEM((span, 4 * share), jnp.float32),
        ],
        name="far",
    )(*shards, m2l_ops, target_cell, l2l_ops)
    pieces = [blocks[0]]
    for length in range(1, REACH + 1):
        for phase in range(2):
            pieces.append(swapped(blocks[2 * length - 1 + phase], length, phase))
    index = (particle_leaf - my_index * cells).reshape(1, -1)
    count = index.shape[1]
    leaf_local, partial = pl.pallas_call(
        functools.partial(near_kernel, share=share, cells=cells),
        out_shape=[
            jax.ShapeDtypeStruct((share, cells), jnp.float32),
            jax.ShapeDtypeStruct((1, count), jnp.float32),
        ],
        in_specs=[vmem] * (BLOCKS + 2),
        out_specs=[vmem] * 2,
        name="near",
    )(*pieces, index, particle_basis)
    sums = from_all(partial.reshape(-1))
    while len(sums) > 1:
        sums = [a + b for a, b in zip(sums[::2], sums[1::2])]
    return (leaf_local, sums[0])


def solution(mesh):
    return jax.shard_map(
        on_device,
        mesh=mesh,
        in_specs=(
            P("coef", "cells"),
            P("coef", "cells"),
            P(None, "coef", None),
            P(None, "coef", None),
            P(None, "cells"),
            P("cells"),
            P("coef", "cells"),
        ),
        out_specs=(P("coef", "cells"), P("cells")),
        check_vma=False,
    )
```

```python
import functools

import jax
import jax.numpy as jnp
from jax import lax
from jax.experimental import pallas as pl
from jax.experimental.pallas import tpu as pltpu
from jax.sharding import PartitionSpec as P

REACH = 2
BLOCKS = 2 * REACH + 1
GROUP = 32
CAP = 256
SLOTS = 2 * REACH * CAP


def swap_steps(index):
    steps = []
    for length in range(1, REACH + 1):
        side = (index // length) % 2
        steps += [length * (1 - 2 * side), length * (2 * side - 1)]
    return steps


def ones_where(mask):
    return jnp.where(mask, 1.0, 0.0).astype(jnp.bfloat16)


def plan_kernel(tgt_ref, row_ref, code_ref, total_ref, padded, *, cells, noff):
    f32, bf16, i32 = jnp.float32, jnp.bfloat16, jnp.int32
    rows = padded.shape[0]
    padded[...] = jnp.full_like(padded, -1)
    padded[:noff, :] = tgt_ref[...]
    target = padded[...]
    rel = target - (lax.axis_index("cells") - REACH) * cells
    above = rel >= (REACH + 1) * cells
    remote = (target >= 0) & ((rel < REACH * cells) | above)
    code = jnp.where(above, rel - cells, rel)
    iota = lambda shape, dim: lax.broadcasted_iota(i32, shape, dim)
    mask = ones_where(remote)
    before = ones_where(iota((cells, cells), 0) < iota((cells, cells), 1))
    within = jnp.dot(mask, before, preferred_element_type=f32)
    counts = jnp.dot(mask, jnp.ones((cells, cells), bf16), preferred_element_type=f32)
    above_rows = ones_where(iota((rows, rows), 1) < iota((rows, rows), 0))
    start = jnp.dot(above_rows, counts.astype(bf16), preferred_element_type=f32).astype(i32)
    counts = counts.astype(i32)
    rank = start + within.astype(i32)
    high = jnp.where(remote, (rank >> 7) + 1, 0)
    low = jnp.where(remote, rank & 127, 0)
    block = jnp.where(remote, code // cells, 0)
    local = jnp.where(remote, code % cells, 0)
    data = jnp.concatenate([high, low, block, local], axis=1).astype(f32).astype(bf16)
    lane = iota((rows, cells), 1)
    offset = iota((rows, cells), 0).astype(f32)
    for j in range(SLOTS // cells):
        slot = lane + j * cells
        hit = (start <= slot) & (slot < start + counts)
        found = lax.dot_general(
            data, ones_where(hit), (((0,), (0,)), ((), ())), preferred_element_type=f32
        )
        slot_c = iota((cells, cells), 1).astype(f32) + float(j * cells)
        mine = found[:cells] * 128.0 + found[cells : 2 * cells] - 128.0 == slot_c
        value = found[2 * cells : 3 * cells] * float(cells) + found[3 * cells :]
        source = iota((cells, cells), 0).astype(f32)
        code_s = jnp.sum(jnp.where(mine, value, 0.0), axis=0, keepdims=True).astype(i32)
        cell_s = jnp.sum(jnp.where(mine, source, 0.0), axis=0, keepdims=True).astype(i32)
        off_s = jnp.sum(jnp.where(hit, offset, 0.0), axis=0, keepdims=True).astype(i32)
        used = jnp.sum(jnp.where(hit, 1.0, 0.0), axis=0, keepdims=True) > 0.0
        at = slice(j * cells, (j + 1) * cells)
        row_ref[:, at] = (off_s >> 1) * cells + cell_s
        code_ref[:, at] = jnp.where(used, code_s + (off_s & 1) * (2 * REACH * cells), -1)
    total_ref[...] = (start + counts)[rows - 8 :, :]


def far_kernel(*refs, share, cells, parents, noff, coefs):
    f32, bf16, i32 = jnp.float32, jnp.bfloat16, jnp.int32
    shards = refs[:coefs]
    ops_ref, tgt_ref, l2l_ref, row_ref, code_ref, total_ref = refs[coefs : coefs + 6]
    outs = refs[coefs + 6 : coefs + 6 + BLOCKS]
    poles, spread_parents, poles_t, hot, rhs, acc, terms, picked, far = refs[coefs + 6 + BLOCKS :]
    cell_index = lax.axis_index("cells")
    coef_index = lax.axis_index("coef")
    lanes = 4 * share
    children = cells // parents
    src = lax.broadcasted_iota(i32, (parents, cells), 0)
    dst = lax.broadcasted_iota(i32, (parents, cells), 1)
    spread = ones_where(dst // children == src)
    for k in range(coefs):
        at = pl.multiple_of((coef_index ^ k) * share, share)
        shard = shards[k][...]
        poles[pl.ds(at, share), :] = shard[:share, :]
        spread_parents[pl.ds(at, share), :] = lax.dot_general(
            shard[share:, :], spread, (((0,), (0,)), ((), ())), preferred_element_type=f32
        )[:share]
    poles_t[...] = poles[...].astype(f32).T.astype(bf16)
    acc[...] = jnp.zeros_like(acc)
    picked[...] = jnp.zeros_like(picked)
    rows = lax.broadcasted_iota(i32, (cells, cells), 0).astype(f32).astype(bf16)
    lane = lax.broadcasted_iota(i32, (cells, lanes), 1)
    is_high = (lane % (2 * share)) < share
    is_even = lane < 2 * share
    one = jnp.ones((cells, cells), bf16)
    zero = jnp.zeros((cells, cells), bf16)

    def chunk(first, count):
        for base in range(0, count, 8):
            size = min(8, count - base)
            local = jnp.clip(tgt_ref[pl.ds(first + base, size), :] - cell_index * cells, -1, cells)
            local = local.astype(f32)
            for j in range(size):
                row = jnp.broadcast_to(local[j : j + 1, :], (cells, cells)).astype(bf16)
                at = (base + j) * cells
                hot[:, at : at + cells] = jnp.where(row == rows, one, zero)
        for j in range(0, count, 4):
            parts = []
            for i in range(0, min(4, count - j), 2):
                even = ops_ref[first + j + i]
                odd = ops_ref[first + j + i + 1] if j + i + 1 < count else even
                parts += [even, even, odd, odd]
            term4 = lax.dot_general(
                poles_t[...],
                jnp.concatenate(parts, axis=0),
                (((1,), (1,)), ((), ())),
                preferred_element_type=f32,
            )
            for i in range(0, min(4, count - j), 2):
                term = term4[:, i * 2 * share : i * 2 * share + lanes]
                high = term.astype(bf16).astype(f32)
                both = jnp.where(is_high, high, term - high)
                at = pl.multiple_of((first + j + i) // 2 * cells, cells)
                terms[pl.ds(at, cells), :] = both
                at = (j + i) * cells
                rhs[at : at + cells, :] = jnp.where(is_even, both, 0.0).astype(bf16)
                if j + i + 1 < count:
                    rhs[at + cells : at + 2 * cells, :] = jnp.where(is_even, 0.0, both).astype(bf16)
        width = count * cells
        acc[...] += jnp.dot(hot[:, :width], rhs[:width, :], preferred_element_type=f32)

    whole = noff // GROUP

    def step(i, carry):
        chunk(pl.multiple_of(i * GROUP, GROUP), GROUP)
        return carry

    lax.fori_loop(0, whole, step, 0)
    if noff % GROUP:
        chunk(whole * GROUP, noff % GROUP)

    def pick(i, carry):
        first = pl.multiple_of(i * 16, 16)
        for j in range(16):
            picked[pl.ds(first + j, 1), :] = terms[pl.ds(row_ref[0, first + j], 1), :]
        return carry

    lax.fori_loop(0, (total_ref[7, 0] + 15) // 16, pick, 0)

    reach_cells = 2 * REACH * cells
    target = lax.broadcasted_iota(i32, (2 * reach_cells, CAP), 0)
    total = jnp.zeros((2 * reach_cells, lanes), f32)
    for j in range(SLOTS // CAP):
        at = slice(j * CAP, (j + 1) * CAP)
        total = total + jnp.dot(
            ones_where(code_ref[:, at] == target),
            picked[at, :].astype(bf16),
            preferred_element_type=f32,
        )
    even_lane = lax.broadcasted_iota(i32, (reach_cells, lanes), 1) < 2 * share
    far[...] = jnp.where(even_lane, total[:reach_cells], total[reach_cells:])

    rep = spread_parents[...]
    octant = lax.broadcasted_iota(i32, rep.shape, 1) % children
    shifted = jnp.zeros((share, cells), f32)
    for o in range(children):
        chosen = jnp.where(octant == o, rep, 0.0).astype(bf16)
        shifted = shifted + jnp.dot(l2l_ref[o], chosen, preferred_element_type=f32)

    def folded(value):
        t = value.T
        return (t[:share] + t[share : 2 * share]) + (t[2 * share : 3 * share] + t[3 * share :])

    outs[0][...] = folded(acc[...]) + shifted
    for out, move in zip(outs[1:], swap_steps(cell_index)):
        block = move + REACH - jnp.where(move > 0, 1, 0)
        at = pl.multiple_of(block * cells, cells)
        out[...] = folded(far[pl.ds(at, cells), :])


def near_kernel(*refs, share, cells):
    pieces = refs[:BLOCKS]
    leaf_ref, basis_ref, out_ref, pot_ref = refs[BLOCKS:]
    f32, bf16 = jnp.float32, jnp.bfloat16
    leaf = pieces[0][...]
    for piece in pieces[1:]:
        leaf = leaf + piece[...]
    out_ref[...] = leaf
    high = leaf.astype(bf16)
    low = (leaf - high.astype(f32)).astype(bf16)
    both = jnp.concatenate([high, low], axis=0)
    count = leaf_ref.shape[1]
    rows = lax.broadcasted_iota(jnp.int32, (cells, count), 0)
    hot = jnp.where(rows == leaf_ref[...], 1.0, 0.0).astype(bf16)
    columns = jnp.dot(both, hot, preferred_element_type=f32)
    columns = columns[:share] + columns[share:]
    pot_ref[...] = jnp.sum(columns * basis_ref[...].astype(f32), axis=0, keepdims=True)


def swapped(value, length, phase):
    count = lax.axis_size("cells")
    pairs = []
    for low in range(count - length):
        if (low // length) % 2 == phase:
            pairs += [(low, low + length), (low + length, low)]
    return lax.ppermute(value, "cells", pairs)


def from_all(value):
    count = lax.axis_size("coef")
    return [value] + [
        lax.ppermute(value, "coef", [(i, i ^ k) for i in range(count)]) for k in range(1, count)
    ]


def on_device(
    multipole, parent_local, m2l_ops, l2l_ops, target_cell, particle_leaf, particle_basis
):
    my_index = lax.axis_index("cells")
    cells = multipole.shape[1]
    parents = parent_local.shape[1]
    coefs = lax.axis_size("coef")
    noff, share, width = m2l_ops.shape
    flipped = jnp.pad(parent_local.T, ((0, 0), (0, cells - share)))
    shards = from_all(jnp.concatenate([multipole, flipped], axis=0))
    vmem = pl.BlockSpec(memory_space=pltpu.VMEM)
    smem = pl.BlockSpec(memory_space=pltpu.SMEM)
    i32 = jnp.int32
    rows, codes, total = pl.pallas_call(
        functools.partial(plan_kernel, cells=cells, noff=noff),
        out_shape=[
            jax.ShapeDtypeStruct((1, SLOTS), i32),
            jax.ShapeDtypeStruct((1, SLOTS), i32),
            jax.ShapeDtypeStruct((8, cells), i32),
        ],
        in_specs=[vmem],
        out_specs=[vmem] * 3,
        scratch_shapes=[pltpu.VMEM((noff + (-noff) % 16, cells), i32)],
        name="plan",
    )(target_cell)
    lanes = 4 * share
    blocks = pl.pallas_call(
        functools.partial(
            far_kernel, share=share, cells=cells, parents=parents, noff=noff, coefs=coefs
        ),
        out_shape=[jax.ShapeDtypeStruct((share, cells), jnp.float32)] * BLOCKS,
        in_specs=[vmem] * (coefs + 3) + [smem, vmem, smem],
        out_specs=[vmem] * BLOCKS,
        scratch_shapes=[
            pltpu.VMEM((width, cells), jnp.bfloat16),
            pltpu.VMEM((width, cells), jnp.float32),
            pltpu.VMEM((cells, width), jnp.bfloat16),
            pltpu.VMEM((cells, GROUP * cells), jnp.bfloat16),
            pltpu.VMEM((GROUP * cells, lanes), jnp.bfloat16),
            pltpu.VMEM((cells, lanes), jnp.float32),
            pltpu.VMEM(((noff + 1) // 2 * cells, lanes), jnp.float32),
            pltpu.VMEM((SLOTS, lanes), jnp.float32),
            pltpu.VMEM((2 * REACH * cells, lanes), jnp.float32),
        ],
        name="far",
    )(*shards, m2l_ops, target_cell, l2l_ops, rows, codes, total)
    pieces = [blocks[0]]
    for length in range(1, REACH + 1):
        for phase in range(2):
            pieces.append(swapped(blocks[2 * length - 1 + phase], length, phase))
    index = (particle_leaf - my_index * cells).reshape(1, -1)
    count = index.shape[1]
    leaf_local, partial = pl.pallas_call(
        functools.partial(near_kernel, share=share, cells=cells),
        out_shape=[
            jax.ShapeDtypeStruct((share, cells), jnp.float32),
            jax.ShapeDtypeStruct((1, count), jnp.float32),
        ],
        in_specs=[vmem] * (BLOCKS + 2),
        out_specs=[vmem] * 2,
        name="near",
    )(*pieces, index, particle_basis)
    sums = from_all(partial.reshape(-1))
    while len(sums) > 1:
        sums = [a + b for a, b in zip(sums[::2], sums[1::2])]
    return (leaf_local, sums[0])


def solution(mesh):
    return jax.shard_map(
        on_device,
        mesh=mesh,
        in_specs=(
            P("coef", "cells"),
            P("coef", "cells"),
            P(None, "coef", None),
            P(None, "coef", None),
            P(None, "cells"),
            P("cells"),
            P("coef", "cells"),
        ),
        out_specs=(P("coef", "cells"), P("cells")),
        check_vma=False,
    )
```

```python
import functools

import jax
import jax.numpy as jnp
from jax import lax
from jax.experimental import pallas as pl
from jax.experimental.pallas import tpu as pltpu
from jax.sharding import PartitionSpec as P

REACH = 2
BLOCKS = 2 * REACH + 1
GROUP = 32
CAP = 256
SLOTS = 2 * REACH * CAP


def swap_steps(index):
    steps = []
    for length in range(1, REACH + 1):
        side = (index // length) % 2
        steps += [length * (1 - 2 * side), length * (2 * side - 1)]
    return steps


def started(sources, targets, sems):
    copies = []
    for i, (source, target) in enumerate(zip(sources, targets)):
        copies.append(pltpu.make_async_copy(source, target, sems.at[i]))
        copies[-1].start()
    return copies


def ones_where(mask):
    return jnp.where(mask, 1.0, 0.0).astype(jnp.bfloat16)


def plan_kernel(tgt_ref, row_ref, code_ref, total_ref, padded, *, cells, noff):
    f32, bf16, i32 = jnp.float32, jnp.bfloat16, jnp.int32
    rows = padded.shape[0]
    padded[...] = jnp.full_like(padded, -1)
    padded[:noff, :] = tgt_ref[...]
    target = padded[...]
    rel = target - (lax.axis_index("cells") - REACH) * cells
    above = rel >= (REACH + 1) * cells
    remote = (target >= 0) & ((rel < REACH * cells) | above)
    code = jnp.where(above, rel - cells, rel)
    iota = lambda shape, dim: lax.broadcasted_iota(i32, shape, dim)
    mask = ones_where(remote)
    before = ones_where(iota((cells, cells), 0) < iota((cells, cells), 1))
    within = jnp.dot(mask, before, preferred_element_type=f32)
    counts = jnp.dot(mask, jnp.ones((cells, cells), bf16), preferred_element_type=f32)
    above_rows = ones_where(iota((rows, rows), 1) < iota((rows, rows), 0))
    start = jnp.dot(above_rows, counts.astype(bf16), preferred_element_type=f32).astype(i32)
    counts = counts.astype(i32)
    rank = start + within.astype(i32)
    high = jnp.where(remote, (rank >> 7) + 1, 0)
    low = jnp.where(remote, rank & 127, 0)
    block = jnp.where(remote, code // cells, 0)
    local = jnp.where(remote, code % cells, 0)
    data = jnp.concatenate([high, low, block, local], axis=1).astype(f32).astype(bf16)
    lane = iota((rows, cells), 1)
    offset = iota((rows, cells), 0).astype(f32)
    for j in range(SLOTS // cells):
        slot = lane + j * cells
        hit = (start <= slot) & (slot < start + counts)
        found = lax.dot_general(
            data, ones_where(hit), (((0,), (0,)), ((), ())), preferred_element_type=f32
        )
        slot_c = iota((cells, cells), 1).astype(f32) + float(j * cells)
        mine = found[:cells] * 128.0 + found[cells : 2 * cells] - 128.0 == slot_c
        value = found[2 * cells : 3 * cells] * float(cells) + found[3 * cells :]
        source = iota((cells, cells), 0).astype(f32)
        code_s = jnp.sum(jnp.where(mine, value, 0.0), axis=0, keepdims=True).astype(i32)
        cell_s = jnp.sum(jnp.where(mine, source, 0.0), axis=0, keepdims=True).astype(i32)
        off_s = jnp.sum(jnp.where(hit, offset, 0.0), axis=0, keepdims=True).astype(i32)
        used = jnp.sum(jnp.where(hit, 1.0, 0.0), axis=0, keepdims=True) > 0.0
        at = slice(j * cells, (j + 1) * cells)
        row_ref[:, at] = (off_s >> 1) * cells + cell_s
        code_ref[:, at] = jnp.where(used, code_s + (off_s & 1) * (2 * REACH * cells), -1)
    total_ref[...] = (start + counts)[rows - 8 :, :]


def far_kernel(*refs, share, cells, parents, noff, coefs):
    f32, bf16, i32 = jnp.float32, jnp.bfloat16, jnp.int32
    row_ref, total_ref = refs[coefs + 4 : coefs + 6]
    outs = refs[coefs + 6 : coefs + 6 + BLOCKS]
    scratch = refs[coefs + 6 + BLOCKS :]
    sems, shard_buf, ops_ref, tgt_ref, l2l_ref, code_ref = scratch[:6]
    poles, spread_parents, poles_t, hot, rhs, acc, terms, picked, far = scratch[6:]
    targets = [shard_buf.at[k] for k in range(coefs)] + [ops_ref, tgt_ref, l2l_ref, code_ref]
    copies = started(refs[: coefs + 4], targets, sems)
    cell_index = lax.axis_index("cells")
    coef_index = lax.axis_index("coef")
    lanes = 4 * share
    children = cells // parents
    src = lax.broadcasted_iota(i32, (parents, cells), 0)
    dst = lax.broadcasted_iota(i32, (parents, cells), 1)
    spread = ones_where(dst // children == src)
    acc[...] = jnp.zeros_like(acc)
    picked[...] = jnp.zeros_like(picked)
    for k in range(coefs):
        copies[k].wait()
    for k in range(coefs):
        at = pl.multiple_of((coef_index ^ k) * share, share)
        shard = shard_buf[k]
        poles[pl.ds(at, share), :] = shard[:share, :]
        spread_parents[pl.ds(at, share), :] = lax.dot_general(
            shard[share:, :], spread, (((0,), (0,)), ((), ())), preferred_element_type=f32
        )[:share]
    poles_t[...] = poles[...].astype(f32).T.astype(bf16)
    for copy in copies[coefs:]:
        copy.wait()
    rows = lax.broadcasted_iota(i32, (cells, cells), 0).astype(f32).astype(bf16)
    lane = lax.broadcasted_iota(i32, (cells, lanes), 1)
    is_high = (lane % (2 * share)) < share
    is_even = lane < 2 * share
    one = jnp.ones((cells, cells), bf16)
    zero = jnp.zeros((cells, cells), bf16)

    def chunk(first, count):
        for base in range(0, count, 8):
            size = min(8, count - base)
            local = jnp.clip(tgt_ref[pl.ds(first + base, size), :] - cell_index * cells, -1, cells)
            local = local.astype(f32)
            for j in range(size):
                row = jnp.broadcast_to(local[j : j + 1, :], (cells, cells)).astype(bf16)
                at = (base + j) * cells
                hot[:, at : at + cells] = jnp.where(row == rows, one, zero)
        for j in range(0, count, 4):
            parts = []
            for i in range(0, min(4, count - j), 2):
                even = ops_ref[first + j + i]
                odd = ops_ref[first + j + i + 1] if j + i + 1 < count else even
                parts += [even, even, odd, odd]
            term4 = lax.dot_general(
                poles_t[...],
                jnp.concatenate(parts, axis=0),
                (((1,), (1,)), ((), ())),
                preferred_element_type=f32,
            )
            for i in range(0, min(4, count - j), 2):
                term = term4[:, i * 2 * share : i * 2 * share + lanes]
                high = term.astype(bf16).astype(f32)
                both = jnp.where(is_high, high, term - high)
                at = pl.multiple_of((first + j + i) // 2 * cells, cells)
                terms[pl.ds(at, cells), :] = both
                at = (j + i) * cells
                rhs[at : at + cells, :] = jnp.where(is_even, both, 0.0).astype(bf16)
                if j + i + 1 < count:
                    rhs[at + cells : at + 2 * cells, :] = jnp.where(is_even, 0.0, both).astype(bf16)
        width = count * cells
        acc[...] += jnp.dot(hot[:, :width], rhs[:width, :], preferred_element_type=f32)

    whole = noff // GROUP

    def step(i, carry):
        chunk(pl.multiple_of(i * GROUP, GROUP), GROUP)
        return carry

    lax.fori_loop(0, whole, step, 0)
    if noff % GROUP:
        chunk(whole * GROUP, noff % GROUP)

    def pick(i, carry):
        first = pl.multiple_of(i * 16, 16)
        for j in range(16):
            picked[pl.ds(first + j, 1), :] = terms[pl.ds(row_ref[0, first + j], 1), :]
        return carry

    lax.fori_loop(0, (total_ref[7, 0] + 15) // 16, pick, 0)

    reach_cells = 2 * REACH * cells
    target = lax.broadcasted_iota(i32, (2 * reach_cells, CAP), 0)
    total = jnp.zeros((2 * reach_cells, lanes), f32)
    for j in range(SLOTS // CAP):
        at = slice(j * CAP, (j + 1) * CAP)
        total = total + jnp.dot(
            ones_where(code_ref[:, at] == target),
            picked[at, :].astype(bf16),
            preferred_element_type=f32,
        )
    even_lane = lax.broadcasted_iota(i32, (reach_cells, lanes), 1) < 2 * share
    far[...] = jnp.where(even_lane, total[:reach_cells], total[reach_cells:])

    rep = spread_parents[...]
    octant = lax.broadcasted_iota(i32, rep.shape, 1) % children
    shifted = jnp.zeros((share, cells), f32)
    for o in range(children):
        chosen = jnp.where(octant == o, rep, 0.0).astype(bf16)
        shifted = shifted + jnp.dot(l2l_ref[o], chosen, preferred_element_type=f32)

    def folded(value):
        t = value.T
        return (t[:share] + t[share : 2 * share]) + (t[2 * share : 3 * share] + t[3 * share :])

    outs[0][...] = folded(acc[...]) + shifted
    for out, move in zip(outs[1:], swap_steps(cell_index)):
        block = move + REACH - jnp.where(move > 0, 1, 0)
        at = pl.multiple_of(block * cells, cells)
        out[...] = folded(far[pl.ds(at, cells), :])


def near_kernel(*refs, share, cells):
    out_ref, pot_ref, sems, pieces, leaf_ref, basis_ref, hot = refs[BLOCKS + 2 :]
    f32, bf16 = jnp.float32, jnp.bfloat16
    targets = [leaf_ref, basis_ref] + [pieces.at[k] for k in range(BLOCKS)]
    copies = started(refs[: BLOCKS + 2], targets, sems)
    copies[0].wait()
    count = leaf_ref.shape[1]
    rows = lax.broadcasted_iota(jnp.int32, (cells, count), 0)
    hot[...] = ones_where(rows == leaf_ref[...] - lax.axis_index("cells") * cells)
    for copy in copies[1:]:
        copy.wait()
    leaf = pieces[0]
    for k in range(1, BLOCKS):
        leaf = leaf + pieces[k]
    out_ref[...] = leaf
    high = leaf.astype(bf16)
    low = (leaf - high.astype(f32)).astype(bf16)
    both = jnp.concatenate([high, low], axis=0)
    columns = jnp.dot(both, hot[...], preferred_element_type=f32)
    columns = columns[:share] + columns[share:]
    pot_ref[...] = jnp.sum(columns * basis_ref[...].astype(f32), axis=0, keepdims=True)


def swapped(value, length, phase):
    count = lax.axis_size("cells")
    pairs = []
    for low in range(count):
        if (low // length) % 2 == phase:
            high = (low + length) % count
            pairs += [(low, high), (high, low)]
    return lax.ppermute(value, "cells", pairs)


def from_all(value):
    count = lax.axis_size("coef")
    return [value] + [
        lax.ppermute(value, "coef", [(i, i ^ k) for i in range(count)]) for k in range(1, count)
    ]


def on_device(
    multipole, parent_local, m2l_ops, l2l_ops, target_cell, particle_leaf, particle_basis
):
    cells = multipole.shape[1]
    parents = parent_local.shape[1]
    coefs = lax.axis_size("coef")
    noff, share, width = m2l_ops.shape
    flipped = jnp.pad(parent_local.T, ((0, 0), (0, cells - share)))
    shards = from_all(jnp.concatenate([multipole, flipped], axis=0))
    vmem = pl.BlockSpec(memory_space=pltpu.VMEM)
    anywhere = pl.BlockSpec(memory_space=pl.ANY)
    smem = pl.BlockSpec(memory_space=pltpu.SMEM)
    i32 = jnp.int32
    rows, codes, total = pl.pallas_call(
        functools.partial(plan_kernel, cells=cells, noff=noff),
        out_shape=[
            jax.ShapeDtypeStruct((1, SLOTS), i32),
            jax.ShapeDtypeStruct((1, SLOTS), i32),
            jax.ShapeDtypeStruct((8, cells), i32),
        ],
        in_specs=[vmem],
        out_specs=[vmem] * 3,
        scratch_shapes=[pltpu.VMEM((noff + (-noff) % 16, cells), i32)],
        name="plan",
    )(target_cell)
    lanes = 4 * share
    blocks = pl.pallas_call(
        functools.partial(
            far_kernel, share=share, cells=cells, parents=parents, noff=noff, coefs=coefs
        ),
        out_shape=[jax.ShapeDtypeStruct((share, cells), jnp.float32)] * BLOCKS,
        in_specs=[anywhere] * (coefs + 4) + [smem, smem],
        out_specs=[vmem] * BLOCKS,
        scratch_shapes=[
            pltpu.SemaphoreType.DMA((coefs + 4,)),
            pltpu.VMEM((coefs,) + shards[0].shape, jnp.bfloat16),
            pltpu.VMEM(m2l_ops.shape, jnp.bfloat16),
            pltpu.VMEM(target_cell.shape, i32),
            pltpu.VMEM(l2l_ops.shape, jnp.bfloat16),
            pltpu.VMEM((1, SLOTS), i32),
            pltpu.VMEM((width, cells), jnp.bfloat16),
            pltpu.VMEM((width, cells), jnp.float32),
            pltpu.VMEM((cells, width), jnp.bfloat16),
            pltpu.VMEM((cells, GROUP * cells), jnp.bfloat16),
            pltpu.VMEM((GROUP * cells, lanes), jnp.bfloat16),
            pltpu.VMEM((cells, lanes), jnp.float32),
            pltpu.VMEM(((noff + 1) // 2 * cells, lanes), jnp.float32),
            pltpu.VMEM((SLOTS, lanes), jnp.float32),
            pltpu.VMEM((2 * REACH * cells, lanes), jnp.float32),
        ],
        name="far",
    )(*shards, m2l_ops, target_cell, l2l_ops, codes, rows, total)
    pieces = [blocks[0]]
    for length in range(1, REACH + 1):
        for phase in range(2):
            pieces.append(swapped(blocks[2 * length - 1 + phase], length, phase))
    index = particle_leaf.reshape(1, -1)
    count = index.shape[1]
    leaf_local, partial = pl.pallas_call(
        functools.partial(near_kernel, share=share, cells=cells),
        out_shape=[
            jax.ShapeDtypeStruct((share, cells), jnp.float32),
            jax.ShapeDtypeStruct((1, count), jnp.float32),
        ],
        in_specs=[anywhere] * (BLOCKS + 2),
        out_specs=[vmem] * 2,
        scratch_shapes=[
            pltpu.SemaphoreType.DMA((BLOCKS + 2,)),
            pltpu.VMEM((BLOCKS, share, cells), jnp.float32),
            pltpu.VMEM((1, count), i32),
            pltpu.VMEM((share, count), jnp.bfloat16),
            pltpu.VMEM((cells, count), jnp.bfloat16),
        ],
        name="near",
    )(index, particle_basis, *pieces)
    sums = from_all(partial.reshape(-1))
    while len(sums) > 1:
        sums = [a + b for a, b in zip(sums[::2], sums[1::2])]
    return (leaf_local, sums[0])


def solution(mesh):
    return jax.shard_map(
        on_device,
        mesh=mesh,
        in_specs=(
            P("coef", "cells"),
            P("coef", "cells"),
            P(None, "coef", None),
            P(None, "coef", None),
            P(None, "cells"),
            P("cells"),
            P("coef", "cells"),
        ),
        out_specs=(P("coef", "cells"), P("cells")),
        check_vma=False,
    )
```

```python
import functools

import jax
import jax.numpy as jnp
from jax import lax
from jax.experimental import pallas as pl
from jax.experimental.pallas import tpu as pltpu
from jax.sharding import PartitionSpec as P

REACH = 2
BLOCKS = 2 * REACH + 1
GROUP = 32
CAP = 256
SLOTS = 2 * REACH * CAP


def swap_steps(index):
    steps = []
    for length in range(1, REACH + 1):
        side = (index // length) % 2
        steps += [length * (1 - 2 * side), length * (2 * side - 1)]
    return steps


def near_by(values):
    return [pltpu.with_memory_space_constraint(value, pltpu.VMEM) for value in values]


def ones_where(mask):
    return jnp.where(mask, 1.0, 0.0).astype(jnp.bfloat16)


def plan_kernel(tgt_ref, row_ref, code_ref, total_ref, padded, *, cells, noff):
    f32, bf16, i32 = jnp.float32, jnp.bfloat16, jnp.int32
    rows = padded.shape[0]
    padded[...] = jnp.full_like(padded, -1)
    padded[:noff, :] = tgt_ref[...]
    target = padded[...]
    rel = target - (lax.axis_index("cells") - REACH) * cells
    above = rel >= (REACH + 1) * cells
    remote = (target >= 0) & ((rel < REACH * cells) | above)
    code = jnp.where(above, rel - cells, rel)
    iota = lambda shape, dim: lax.broadcasted_iota(i32, shape, dim)
    mask = ones_where(remote)
    before = ones_where(iota((cells, cells), 0) < iota((cells, cells), 1))
    within = jnp.dot(mask, before, preferred_element_type=f32)
    counts = jnp.dot(mask, jnp.ones((cells, cells), bf16), preferred_element_type=f32)
    above_rows = ones_where(iota((rows, rows), 1) < iota((rows, rows), 0))
    start = jnp.dot(above_rows, counts.astype(bf16), preferred_element_type=f32).astype(i32)
    counts = counts.astype(i32)
    rank = start + within.astype(i32)
    high = jnp.where(remote, (rank >> 7) + 1, 0)
    low = jnp.where(remote, rank & 127, 0)
    block = jnp.where(remote, code // cells, 0)
    local = jnp.where(remote, code % cells, 0)
    data = jnp.concatenate([high, low, block, local], axis=1).astype(f32).astype(bf16)
    lane = iota((rows, cells), 1)
    offset = iota((rows, cells), 0).astype(f32)
    for j in range(SLOTS // cells):
        slot = lane + j * cells
        hit = (start <= slot) & (slot < start + counts)
        found = lax.dot_general(
            data, ones_where(hit), (((0,), (0,)), ((), ())), preferred_element_type=f32
        )
        slot_c = iota((cells, cells), 1).astype(f32) + float(j * cells)
        mine = found[:cells] * 128.0 + found[cells : 2 * cells] - 128.0 == slot_c
        value = found[2 * cells : 3 * cells] * float(cells) + found[3 * cells :]
        source = iota((cells, cells), 0).astype(f32)
        code_s = jnp.sum(jnp.where(mine, value, 0.0), axis=0, keepdims=True).astype(i32)
        cell_s = jnp.sum(jnp.where(mine, source, 0.0), axis=0, keepdims=True).astype(i32)
        off_s = jnp.sum(jnp.where(hit, offset, 0.0), axis=0, keepdims=True).astype(i32)
        used = jnp.sum(jnp.where(hit, 1.0, 0.0), axis=0, keepdims=True) > 0.0
        at = slice(j * cells, (j + 1) * cells)
        row_ref[:, at] = (off_s >> 1) * cells + cell_s
        code_ref[:, at] = jnp.where(used, code_s + (off_s & 1) * (2 * REACH * cells), -1)
    total_ref[...] = (start + counts)[rows - 8 :, :]


def far_kernel(*refs, share, cells, parents, noff, coefs):
    f32, bf16, i32 = jnp.float32, jnp.bfloat16, jnp.int32
    row_ref, total_ref = refs[coefs + 4 : coefs + 6]
    outs = refs[coefs + 6 : coefs + 6 + BLOCKS]
    scratch = refs[coefs + 6 + BLOCKS :]
    shards = refs[:coefs]
    ops_ref, tgt_ref, l2l_ref, code_ref = refs[coefs : coefs + 4]
    poles, spread_parents, poles_t, hot, rhs, acc, terms, picked, far = scratch
    cell_index = lax.axis_index("cells")
    coef_index = lax.axis_index("coef")
    lanes = 4 * share
    children = cells // parents
    src = lax.broadcasted_iota(i32, (parents, cells), 0)
    dst = lax.broadcasted_iota(i32, (parents, cells), 1)
    spread = ones_where(dst // children == src)
    acc[...] = jnp.zeros_like(acc)
    picked[...] = jnp.zeros_like(picked)
    for k in range(coefs):
        at = pl.multiple_of((coef_index ^ k) * share, share)
        shard = shards[k][...]
        poles[pl.ds(at, share), :] = shard[:share, :]
        spread_parents[pl.ds(at, share), :] = lax.dot_general(
            shard[share:, :], spread, (((0,), (0,)), ((), ())), preferred_element_type=f32
        )[:share]
    poles_t[...] = poles[...].astype(f32).T.astype(bf16)
    rows = lax.broadcasted_iota(i32, (cells, cells), 0).astype(f32).astype(bf16)
    lane = lax.broadcasted_iota(i32, (cells, lanes), 1)
    is_high = (lane % (2 * share)) < share
    is_even = lane < 2 * share
    one = jnp.ones((cells, cells), bf16)
    zero = jnp.zeros((cells, cells), bf16)

    def chunk(first, count):
        for base in range(0, count, 8):
            size = min(8, count - base)
            local = jnp.clip(tgt_ref[pl.ds(first + base, size), :] - cell_index * cells, -1, cells)
            local = local.astype(f32)
            for j in range(size):
                row = jnp.broadcast_to(local[j : j + 1, :], (cells, cells)).astype(bf16)
                at = (base + j) * cells
                hot[:, at : at + cells] = jnp.where(row == rows, one, zero)
        for j in range(0, count, 4):
            parts = []
            for i in range(0, min(4, count - j), 2):
                even = ops_ref[first + j + i]
                odd = ops_ref[first + j + i + 1] if j + i + 1 < count else even
                parts += [even, even, odd, odd]
            term4 = lax.dot_general(
                poles_t[...],
                jnp.concatenate(parts, axis=0),
                (((1,), (1,)), ((), ())),
                preferred_element_type=f32,
            )
            for i in range(0, min(4, count - j), 2):
                term = term4[:, i * 2 * share : i * 2 * share + lanes]
                high = term.astype(bf16).astype(f32)
                both = jnp.where(is_high, high, term - high)
                at = pl.multiple_of((first + j + i) // 2 * cells, cells)
                terms[pl.ds(at, cells), :] = both
                at = (j + i) * cells
                rhs[at : at + cells, :] = jnp.where(is_even, both, 0.0).astype(bf16)
                if j + i + 1 < count:
                    rhs[at + cells : at + 2 * cells, :] = jnp.where(is_even, 0.0, both).astype(bf16)
        width = count * cells
        acc[...] += jnp.dot(hot[:, :width], rhs[:width, :], preferred_element_type=f32)

    whole = noff // GROUP

    def step(i, carry):
        chunk(pl.multiple_of(i * GROUP, GROUP), GROUP)
        return carry

    lax.fori_loop(0, whole, step, 0)
    if noff % GROUP:
        chunk(whole * GROUP, noff % GROUP)

    def pick(i, carry):
        first = pl.multiple_of(i * 16, 16)
        for j in range(16):
            picked[pl.ds(first + j, 1), :] = terms[pl.ds(row_ref[0, first + j], 1), :]
        return carry

    lax.fori_loop(0, (total_ref[7, 0] + 15) // 16, pick, 0)

    reach_cells = 2 * REACH * cells
    target = lax.broadcasted_iota(i32, (2 * reach_cells, CAP), 0)
    total = jnp.zeros((2 * reach_cells, lanes), f32)
    for j in range(SLOTS // CAP):
        at = slice(j * CAP, (j + 1) * CAP)
        total = total + jnp.dot(
            ones_where(code_ref[:, at] == target),
            picked[at, :].astype(bf16),
            preferred_element_type=f32,
        )
    even_lane = lax.broadcasted_iota(i32, (reach_cells, lanes), 1) < 2 * share
    far[...] = jnp.where(even_lane, total[:reach_cells], total[reach_cells:])

    rep = spread_parents[...]
    octant = lax.broadcasted_iota(i32, rep.shape, 1) % children
    shifted = jnp.zeros((share, cells), f32)
    for o in range(children):
        chosen = jnp.where(octant == o, rep, 0.0).astype(bf16)
        shifted = shifted + jnp.dot(l2l_ref[o], chosen, preferred_element_type=f32)

    def folded(value):
        t = value.T
        return (t[:share] + t[share : 2 * share]) + (t[2 * share : 3 * share] + t[3 * share :])

    outs[0][...] = folded(acc[...]) + shifted
    for out, move in zip(outs[1:], swap_steps(cell_index)):
        block = move + REACH - jnp.where(move > 0, 1, 0)
        at = pl.multiple_of(block * cells, cells)
        out[...] = folded(far[pl.ds(at, cells), :])


def near_kernel(*refs, share, cells):
    leaf_ref, basis_ref = refs[:2]
    pieces = refs[2 : BLOCKS + 2]
    out_ref, pot_ref = refs[BLOCKS + 2 :]
    f32, bf16 = jnp.float32, jnp.bfloat16
    count = leaf_ref.shape[1]
    rows = lax.broadcasted_iota(jnp.int32, (cells, count), 0)
    hot = ones_where(rows == leaf_ref[...] - lax.axis_index("cells") * cells)
    leaf = pieces[0][...]
    for piece in pieces[1:]:
        leaf = leaf + piece[...]
    out_ref[...] = leaf
    high = leaf.astype(bf16)
    low = (leaf - high.astype(f32)).astype(bf16)
    both = jnp.concatenate([high, low], axis=0)
    columns = jnp.dot(both, hot, preferred_element_type=f32)
    columns = columns[:share] + columns[share:]
    pot_ref[...] = jnp.sum(columns * basis_ref[...].astype(f32), axis=0, keepdims=True)


def swapped(value, length, phase):
    count = lax.axis_size("cells")
    pairs = []
    for low in range(count):
        if (low // length) % 2 == phase:
            high = (low + length) % count
            pairs += [(low, high), (high, low)]
    return lax.ppermute(value, "cells", pairs)


def from_all(value):
    count = lax.axis_size("coef")
    return [value] + [
        lax.ppermute(value, "coef", [(i, i ^ k) for i in range(count)]) for k in range(1, count)
    ]


def on_device(
    multipole, parent_local, m2l_ops, l2l_ops, target_cell, particle_leaf, particle_basis
):
    cells = multipole.shape[1]
    parents = parent_local.shape[1]
    coefs = lax.axis_size("coef")
    noff, share, width = m2l_ops.shape
    flipped = jnp.pad(parent_local.T, ((0, 0), (0, cells - share)))
    shards = from_all(jnp.concatenate([multipole, flipped], axis=0))
    vmem = pl.BlockSpec(memory_space=pltpu.VMEM)
    smem = pl.BlockSpec(memory_space=pltpu.SMEM)
    i32 = jnp.int32
    rows, codes, total = pl.pallas_call(
        functools.partial(plan_kernel, cells=cells, noff=noff),
        out_shape=[
            jax.ShapeDtypeStruct((1, SLOTS), i32),
            jax.ShapeDtypeStruct((1, SLOTS), i32),
            jax.ShapeDtypeStruct((8, cells), i32),
        ],
        in_specs=[vmem],
        out_specs=[vmem] * 3,
        scratch_shapes=[pltpu.VMEM((noff + (-noff) % 16, cells), i32)],
        name="plan",
    )(target_cell)
    lanes = 4 * share
    blocks = pl.pallas_call(
        functools.partial(
            far_kernel, share=share, cells=cells, parents=parents, noff=noff, coefs=coefs
        ),
        out_shape=[pltpu.VMEM((share, cells), jnp.float32)] * BLOCKS,
        in_specs=[vmem] * (coefs + 4) + [smem, smem],
        out_specs=[vmem] * BLOCKS,
        scratch_shapes=[
            pltpu.VMEM((width, cells), jnp.bfloat16),
            pltpu.VMEM((width, cells), jnp.float32),
            pltpu.VMEM((cells, width), jnp.bfloat16),
            pltpu.VMEM((cells, GROUP * cells), jnp.bfloat16),
            pltpu.VMEM((GROUP * cells, lanes), jnp.bfloat16),
            pltpu.VMEM((cells, lanes), jnp.float32),
            pltpu.VMEM(((noff + 1) // 2 * cells, lanes), jnp.float32),
            pltpu.VMEM((SLOTS, lanes), jnp.float32),
            pltpu.VMEM((2 * REACH * cells, lanes), jnp.float32),
        ],
        name="far",
    )(*near_by(shards), m2l_ops, target_cell, l2l_ops, codes, rows, total)
    pieces = [blocks[0]]
    for length in range(1, REACH + 1):
        for phase in range(2):
            pieces.append(swapped(blocks[2 * length - 1 + phase], length, phase))
    index = particle_leaf.reshape(1, -1)
    count = index.shape[1]
    leaf_local, partial = pl.pallas_call(
        functools.partial(near_kernel, share=share, cells=cells),
        out_shape=[
            jax.ShapeDtypeStruct((share, cells), jnp.float32),
            pltpu.VMEM((1, count), jnp.float32),
        ],
        in_specs=[vmem] * (BLOCKS + 2),
        out_specs=[vmem] * 2,
        name="near",
    )(*near_by([index, particle_basis] + pieces))
    sums = from_all(partial.reshape(-1))
    while len(sums) > 1:
        sums = [a + b for a, b in zip(sums[::2], sums[1::2])]
    return (leaf_local, sums[0])


def solution(mesh):
    return jax.shard_map(
        on_device,
        mesh=mesh,
        in_specs=(
            P("coef", "cells"),
            P("coef", "cells"),
            P(None, "coef", None),
            P(None, "coef", None),
            P(None, "cells"),
            P("cells"),
            P("coef", "cells"),
        ),
        out_specs=(P("coef", "cells"), P("cells")),
        check_vma=False,
    )
```
